32 devices in a mesh: groups: 2 (over y), vocab: 16 (over z, x, core).
Axes of the slice: x: 2, y: 2, z: 4, core: 2. Of those that a mesh axis runs over, the one named last changes fastest.
Arguments:
- hidden: bfloat16 [512, 1280], P(('groups', 'vocab')), parts along dimension 0, may hold values from -320 to 320
- embedding: bfloat16 [6144, 1280], P('vocab'), may hold values from -0.15625 to 0.15625
- prev_tokens: int32 [2, 512], P(None, 'groups'), parts along dimension 1, may hold values from 0 to 6143, as said below
- last_stamp: int32 [512], P('groups'), parts along dimension 0, may hold values from -1 to 1500, as said below
- sample_begin: int32 [512], P('groups'), parts along dimension 0, may hold values from 1 to 4
- seq_length: int32 [512], P('groups'), parts along dimension 0, may hold values from 1 to 9, as said below
- chosen: int32 [5, 512], P(None, 'groups'), parts along dimension 1, may hold values from 0 to 6143
Outputs:
- picked_logprob: float32 [5, 512], P(None, ('groups', 'vocab')), parts along dimension 1
- stamp_logprob: float32 [512], P(('groups', 'vocab')), parts along dimension 0
The draws below stay inside these ranges and needn't reach their ends.
There are 2 independent parts, one for each index of `groups`. The reference program is written for one: setup_inputs(seed, part) draws one part's arguments, and reference() takes and returns one part's arrays. A program takes and returns all parts, laid end to end along the dimension named above; an argument that names none is the same for every part. Nothing has to cross between parts.
Inputs may be any that keep to these rules, and one draw needn't show every extreme that they name: prev_tokens[1, r] is row r's latest token and prev_tokens[0, r] the one before; ids at or above 4643 are timestamps. `last_stamp`: index among the 1501 timestamps of the latest timestamp token sampled since the row's sample begin, -1 if none; equal to the latest token's index when that token is a timestamp and was sampled. `seq_length`: at least the row's sample_begin and at most sample_begin + 5.
All inputs are finite; a program needn't handle non-finite values.
Results may differ from the reference program's by a relative error of at most 0.0003.
Values may be sent and summed in bfloat16 or wider, within the bound.
A program may use at most 64 MiB of HBM per device.

```python
import math
import jax
import jax.numpy as jnp
from jax import lax

D = 1280
VOCAB = 6144
TSN = 1501
SPECIALS = 108
INITIAL = 50
NSEL = 5
ROWS = 256


def history(key):
    keys = jax.random.split(jax.random.fold_in(key, 4242), 8)
    stamp_begin = VOCAB - TSN
    begin = jax.random.randint(keys[0], (ROWS,), 1, 5)
    generated = jax.random.randint(keys[1], (ROWS,), 0, 6)
    last_flag = jax.random.randint(keys[2], (ROWS,), 0, 2) == 1
    before_flag = jax.random.randint(keys[3], (ROWS,), 0, 2) == 1
    last_index = jax.random.randint(keys[4], (ROWS,), 0, TSN)
    before_index = jax.random.randint(keys[5], (ROWS,), 0, TSN)
    text_tokens = jax.random.randint(keys[6], (2, ROWS), 0, stamp_begin - SPECIALS)
    earlier = jnp.maximum(jax.random.randint(keys[7], (ROWS,), -TSN, TSN), -1)
    last_is = last_flag & (generated >= 1)
    before_is = before_flag & (generated >= 2)
    last_token = jnp.where(last_is, stamp_begin + last_index, text_tokens[1])
    before_token = jnp.where(before_is, stamp_begin + before_index, text_tokens[0])
    stamp = jnp.where(last_is, last_index, jnp.where(before_is, before_index, jnp.where(generated >= 3, earlier, -1)))
    tokens = jnp.stack([before_token, last_token]).astype(jnp.int32)
    return (tokens, stamp.astype(jnp.int32), begin.astype(jnp.int32), (begin + generated).astype(jnp.int32))


def draw_prev_tokens(key, part):
    return history(key)[0]


def draw_last_stamp(key, part):
    return history(key)[1]


def draw_sample_begin(key, part):
    return history(key)[2]


def draw_seq_length(key, part):
    return history(key)[3]


def draw_hidden(key, part):
    first, second = jax.random.split(key)
    values = jnp.clip(3.0 * jax.random.normal(first, (ROWS, D), jnp.float32), -18.0, 18.0)
    return values.astype(jnp.bfloat16)


def touch_ends(drawn, rng, smallest, high):
    longest = drawn.shape.index(max(drawn.shape))
    spots = []
    for shift in (0, 1):
        where = [jax.random.randint(jax.random.fold_in(rng, axis), (), 0, length) for axis, length in enumerate(drawn.shape)]
        where[longest] = (where[longest] + shift) % drawn.shape[longest]
        spots.append(tuple(where))
    return drawn.at[spots[0]].set(smallest).at[spots[1]].set(high)


def block_levels(own_key, extent, pieces, smallest, high):
    def one(dim, shards_of):
        steps = jax.random.uniform(jax.random.fold_in(jax.random.fold_in(own_key, 6), dim), (shards_of,), jnp.float32, smallest / len(pieces), high / len(pieces))
        return jnp.repeat(jnp.exp(steps), extent[dim] // shards_of).reshape((-1,) + (1,) * (len(extent) - dim - 1))

    factor_of = one(*pieces[0])
    for cut in pieces[1:]:
        factor_of = factor_of * one(*cut)
    return factor_of


def bell_draw(rng, extent, width, most, shards=(), kind=jnp.bfloat16):
    gain = block_levels(rng, extent, shards, -0.22, 0.18) if shards else 1.0
    array = jax.random.normal(rng, extent, jnp.float32) * width * gain
    return jnp.minimum(jnp.maximum(array, -most), most).astype(kind)


def setup_inputs(seed: int = 0, part: int = 0) -> dict:
    streams_of = jax.random.split(jax.random.key(seed), 8)
    own_keys = jax.random.split(jax.random.fold_in(streams_of[7], part), 8)
    return {
        "hidden": draw_hidden(jax.random.fold_in(jax.random.fold_in(streams_of[7], part), 71), part),
        "embedding": bell_draw(streams_of[1], (VOCAB, D), D ** -0.5, 0.15625, ((0, 16),)),
        "prev_tokens": draw_prev_tokens(jax.random.fold_in(jax.random.fold_in(streams_of[7], part), 71), part),
        "last_stamp": draw_last_stamp(jax.random.fold_in(jax.random.fold_in(streams_of[7], part), 71), part),
        "sample_begin": draw_sample_begin(jax.random.fold_in(jax.random.fold_in(streams_of[7], part), 71), part),
        "seq_length": draw_seq_length(jax.random.fold_in(jax.random.fold_in(streams_of[7], part), 71), part),
        "chosen": touch_ends(jax.random.randint(own_keys[6], (NSEL, ROWS), 0, VOCAB), jax.random.fold_in(own_keys[6], 1), 0, VOCAB - 1).astype(jnp.int32),
    }


MASK_VALUE = -1.0e9
SLOPE = 4.0
FLOOR = -30.0


def rule_mask(columns, prev_tokens, last_stamp, sample_begin, seq_length, stamp_begin):
    generated = seq_length - sample_begin
    last_is = (generated >= 1) & (prev_tokens[1] >= stamp_begin)
    before_is = (generated < 2) | (prev_tokens[0] >= stamp_begin)
    column = columns[None, :]
    is_stamp = column >= stamp_begin
    offset = column - stamp_begin
    masked = column == stamp_begin - 1
    masked = masked | ((last_is & before_is)[:, None] & is_stamp)
    masked = masked | ((last_is & ~before_is)[:, None] & (column < stamp_begin - SPECIALS))
    bound = last_stamp + jnp.where(last_is & ~before_is, 0, 1).astype(jnp.int32)
    masked = masked | (is_stamp & (offset < bound[:, None]) & (last_stamp >= 0)[:, None])
    begin = (generated == 0)[:, None]
    masked = masked | (begin & (column < stamp_begin))
    masked = masked | (begin & is_stamp & (offset > INITIAL))
    return masked


def finalize(text_max, text_total, stamp_max, stamp_total, picked, chosen, stamp_begin):
    text_lse = text_max + jnp.log(text_total)
    stamp_lse = stamp_max + jnp.log(stamp_total)
    penalty = SLOPE * jnp.maximum(stamp_lse - text_max, 0.0)
    shifted = text_lse - penalty
    larger = jnp.maximum(shifted, stamp_lse)
    total = larger + jnp.log(jnp.exp(shifted - larger) + jnp.exp(stamp_lse - larger))
    adjusted = picked - jnp.where(chosen < stamp_begin, penalty[None, :], 0.0) - total[None, :]
    return jnp.maximum(adjusted, FLOOR), jnp.maximum(stamp_lse - total, FLOOR)


def reference(hidden, embedding, prev_tokens, last_stamp, sample_begin, seq_length, chosen):
    stamp_begin = VOCAB - TSN
    columns = jnp.arange(VOCAB, dtype=jnp.int32)
    is_text = columns < stamp_begin
    block = math.gcd(ROWS, 256)
    blocks = ROWS // block

    def one_block(index):
        start = (index * block).astype(jnp.int32)
        rows = lax.dynamic_slice_in_dim(hidden, start, block, 0)
        prev = lax.dynamic_slice_in_dim(prev_tokens, start, block, 1)
        stamp = lax.dynamic_slice_in_dim(last_stamp, start, block, 0)
        begin = lax.dynamic_slice_in_dim(sample_begin, start, block, 0)
        length = lax.dynamic_slice_in_dim(seq_length, start, block, 0)
        pick = lax.dynamic_slice_in_dim(chosen, start, block, 1)
        logits = lax.dot_general(rows, embedding, (((1,), (1,)), ((), ())), preferred_element_type=jnp.float32)
        masked = rule_mask(columns, prev, stamp, begin, length, stamp_begin)
        values = jnp.where(masked, MASK_VALUE, logits)
        text_max = jnp.max(jnp.where(is_text, values, -jnp.inf), axis=1)
        text_total = jnp.sum(jnp.where(is_text, jnp.exp(values - text_max[:, None]), 0.0), axis=1)
        stamp_max = jnp.max(jnp.where(is_text, -jnp.inf, values), axis=1)
        stamp_total = jnp.sum(jnp.where(is_text, 0.0, jnp.exp(values - stamp_max[:, None])), axis=1)
        picked = jnp.take_along_axis(values, pick.T, axis=1).T
        return text_max, text_total, stamp_max, stamp_total, picked

    text_max, text_total, stamp_max, stamp_total, picked = lax.map(one_block, jnp.arange(blocks, dtype=jnp.int32))
    picked = jnp.transpose(picked, (1, 0, 2)).reshape(NSEL, ROWS)
    return finalize(text_max.reshape(ROWS), text_total.reshape(ROWS), stamp_max.reshape(ROWS), stamp_total.reshape(ROWS), picked, chosen, stamp_begin)
```

```python
import functools
import math

import jax
import jax.numpy as jnp
from jax import lax
from jax.experimental import pallas as pl
from jax.experimental.pallas import tpu as pltpu
from jax.sharding import PartitionSpec as P

TSN = 1501
SPECIALS = 108
INITIAL = 50

MASK_VALUE = -1000000000.0
EMPTY_VALUE = -3000000000.0
SLOPE = 4.0
FLOOR = -30.0
BIG = 1 << 30
LANES = 128
MESH = pl.DeviceIdType.MESH


def kernel(
    count,
    hidden_ref,
    table_ref,
    prev_ref,
    stamp_ref,
    begin_ref,
    length_ref,
    chosen_ref,
    picked_ref,
    stamp_out_ref,
    rows_all,
    table,
    stats,
    gathered,
    table_sem,
    own_sem,
    send_sem,
    recv_sem,
    stat_send_sem,
    stat_recv_sem,
):
    row_dev = hidden_ref.shape[0]
    width = table_ref.shape[0]
    nsel = chosen_ref.shape[0]
    rows_here = count * row_dev
    stamp_begin = width * count - TSN
    group = lax.axis_index("groups")
    me = lax.axis_index("vocab")
    line = count // 4
    z, x, c = me // 4, (me // 2) % 2, me % 2

    def at(zz, xx, cc):
        return (zz * 2 + xx) * 2 + cc

    def slot(owner):
        return rows_all.at[pl.ds(pl.multiple_of(owner * row_dev, row_dev), row_dev)]

    load_own = pltpu.make_async_copy(hidden_ref, slot(me), own_sem)
    load_own.start()
    load_table = pltpu.make_async_copy(table_ref, table, table_sem)
    load_table.start()

    barrier = pltpu.get_barrier_semaphore()
    for i in range(1, count):
        pl.semaphore_signal(
            barrier, inc=1, device_id=(group, (me + i) % count), device_id_type=MESH
        )

    sends = []

    def send(owner, target):
        copy = pltpu.make_async_remote_copy(
            src_ref=slot(owner),
            dst_ref=slot(owner),
            send_sem=send_sem.at[len(sends)],
            recv_sem=recv_sem.at[owner],
            device_id=(group, target),
            device_id_type=MESH,
        )
        copy.start()
        sends.append(copy)

    def arrive(owner):
        pltpu.make_async_remote_copy(
            src_ref=slot(owner),
            dst_ref=slot(owner),
            send_sem=send_sem.at[0],
            recv_sem=recv_sem.at[owner],
            device_id=(group, (me + 1) % count),
            device_id_type=MESH,
        ).wait_recv()

    load_own.wait()
    pl.semaphore_wait(barrier, count - 1)
    order = sorted(range(1, line), key=lambda i: -min(i, line - i))
    across = at(z, 1 - x, c)
    partner = at(z, x, 1 - c)
    for i in order:
        send(me, at((z + i) % line, x, c))
    send(me, across)
    send(me, partner)
    for i in order:
        owner = at((z + line - i) % line, x, c)
        arrive(owner)
        send(owner, across)
        send(owner, partner)
    for i in [0] + order:
        owner = at((z + line - i) % line, 1 - x, c)
        arrive(owner)
        send(owner, partner)
    for i in [0] + order:
        arrive(at((z + line - i) % line, x, 1 - c))
    for i in [0] + order:
        arrive(at((z + line - i) % line, 1 - x, 1 - c))
    load_table.wait()

    block = math.gcd(rows_here, 256)
    column = me * width + lax.broadcasted_iota(jnp.int32, (width, block), 0)
    is_text = column < stamp_begin

    def one_block(number):
        at_row = number * block
        if not isinstance(number, int):
            at_row = pl.multiple_of(at_row, block)
        lanes = pl.ds(at_row, block)
        logits = lax.dot_general(
            table[...],
            rows_all[lanes, :],
            (((1,), (1,)), ((), ())),
            preferred_element_type=jnp.float32,
        )
        generated = length_ref[:, lanes] - begin_ref[:, lanes]
        last_stamp = stamp_ref[:, lanes]
        last_is = (generated >= 1) & (prev_ref[1:2, lanes] >= stamp_begin)
        before_is = (generated < 2) | (prev_ref[0:1, lanes] >= stamp_begin)
        opened = last_is & jnp.logical_not(before_is)
        closed = last_is & before_is
        first = generated == 0
        text_low = jnp.where(first, BIG, jnp.where(opened, stamp_begin - SPECIALS, 0))
        bound = last_stamp + jnp.where(opened, 0, 1)
        stamp_low = jnp.where(
            closed, BIG, stamp_begin + jnp.where(last_stamp >= 0, bound, 0)
        )
        stamp_high = jnp.where(first, stamp_begin + INITIAL + 1, BIG)
        low = jnp.where(is_text, text_low, stamp_low)
        high = jnp.where(is_text, stamp_begin - 1, stamp_high)
        values = jnp.where((column >= low) & (column < high), logits, MASK_VALUE)
        text_max = jnp.max(jnp.where(is_text, values, EMPTY_VALUE), axis=0, keepdims=True)
        stamp_max = jnp.max(jnp.where(is_text, EMPTY_VALUE, values), axis=0, keepdims=True)
        powers = jnp.exp(values - jnp.where(is_text, text_max, stamp_max))
        text_total = jnp.sum(jnp.where(is_text, powers, 0.0), axis=0, keepdims=True)
        stamp_total = jnp.sum(jnp.where(is_text, 0.0, powers), axis=0, keepdims=True)
        text_lse = jnp.where(text_total > 0.0, text_max + jnp.log(text_total), EMPTY_VALUE)
        stamp_lse = jnp.where(stamp_total > 0.0, stamp_max + jnp.log(stamp_total), EMPTY_VALUE)
        found = [
            jnp.sum(
                jnp.where(column == chosen_ref[k : k + 1, lanes], values, 0.0),
                axis=0,
                keepdims=True,
            )
            for k in range(nsel)
        ]
        lines = [text_max, text_lse, stamp_lse] + found
        lines += [jnp.zeros_like(text_max)] * (8 - len(lines))
        result = jnp.concatenate(lines, axis=0)
        for part in range(block // LANES):
            stats[number * (block // LANES) + part] = result[:, part * LANES : (part + 1) * LANES]

    if rows_here == block:
        one_block(0)
    else:
        pl.loop(0, rows_here // block)(one_block)

    def stat_copy(i):
        target = (me + i) % count
        return pltpu.make_async_remote_copy(
            src_ref=stats.at[(target * row_dev) // LANES],
            dst_ref=gathered.at[me],
            send_sem=stat_send_sem.at[i],
            recv_sem=stat_recv_sem.at[me],
            device_id=(group, target),
            device_id_type=MESH,
        )

    stat_sends = [stat_copy(i) for i in range(1, count)]
    for copy in stat_sends:
        copy.start()
    chunk = (me * row_dev) // LANES
    gathered[me] = stats[chunk]
    for copy in sends:
        copy.wait_send()
    for i in range(1, count):
        source = (me + count - i) % count
        pltpu.make_async_remote_copy(
            src_ref=stats.at[0],
            dst_ref=gathered.at[source],
            send_sem=stat_send_sem.at[0],
            recv_sem=stat_recv_sem.at[source],
            device_id=(group, (me + 1) % count),
            device_id_type=MESH,
        ).wait_recv()

    tiles = gathered[...]
    top = jnp.max(tiles, axis=0)
    lse = top + jnp.log(jnp.sum(jnp.exp(tiles - top[None]), axis=0))
    picked = jnp.sum(tiles, axis=0)[3 : 3 + nsel]
    text_max, text_lse, stamp_lse = top[0:1], lse[1:2], lse[2:3]
    penalty = SLOPE * jnp.maximum(stamp_lse - text_max, 0.0)
    shifted = text_lse - penalty
    larger = jnp.maximum(shifted, stamp_lse)
    total = larger + jnp.log(jnp.exp(shifted - larger) + jnp.exp(stamp_lse - larger))
    own_chosen = chosen_ref[:, pl.ds(pl.multiple_of(chunk * LANES, LANES), LANES)]
    adjusted = picked - jnp.where(own_chosen < stamp_begin, penalty, 0.0) - total
    final = jnp.concatenate(
        [adjusted, stamp_lse - total] + [jnp.zeros_like(total)] * (7 - nsel), axis=0
    )
    final = jnp.maximum(final, FLOOR)
    offset = (me * row_dev) % LANES
    final = pltpu.roll(final, (LANES - offset) % LANES, 1)
    picked_ref[...] = final[:nsel, :row_dev]
    stamp_out_ref[...] = final[nsel : nsel + 1, :row_dev]
    for copy in stat_sends:
        copy.wait_send()


def per_device(hidden, embedding, prev_tokens, last_stamp, sample_begin, seq_length, chosen):
    count = lax.axis_size("vocab")
    row_dev, depth = hidden.shape
    width = embedding.shape[0]
    nsel = chosen.shape[0]
    rows_here = count * row_dev
    anywhere = pl.BlockSpec(memory_space=pl.ANY)
    local = pl.BlockSpec(memory_space=pltpu.VMEM)
    picked, stamp = pl.pallas_call(
        functools.partial(kernel, count),
        out_shape=(
            jax.ShapeDtypeStruct((nsel, row_dev), jnp.float32),
            jax.ShapeDtypeStruct((1, row_dev), jnp.float32),
        ),
        in_specs=[anywhere, anywhere] + [local] * 5,
        out_specs=(local, local),
        scratch_shapes=[
            pltpu.VMEM((rows_here, depth), hidden.dtype),
            pltpu.VMEM((width, depth), embedding.dtype),
            pltpu.VMEM((rows_here // LANES, 8, LANES), jnp.float32),
            pltpu.VMEM((count, 8, LANES), jnp.float32),
            pltpu.SemaphoreType.DMA,
            pltpu.SemaphoreType.DMA,
            pltpu.SemaphoreType.DMA((count,)),
            pltpu.SemaphoreType.DMA((count,)),
            pltpu.SemaphoreType.DMA((count,)),
            pltpu.SemaphoreType.DMA((count,)),
        ],
        compiler_params=pltpu.CompilerParams(collective_id=0, has_side_effects=True),
        name="decode_step",
    )(
        hidden,
        embedding,
        prev_tokens,
        last_stamp[None, :],
        sample_begin[None, :],
        seq_length[None, :],
        chosen,
    )
    return picked, stamp[0]


def solution(mesh):
    placed = (
        P(("groups", "vocab"), None),
        P("vocab", None),
        P(None, "groups"),
        P("groups"),
        P("groups"),
        P("groups"),
        P(None, "groups"),
    )
    return jax.shard_map(
        per_device,
        mesh=mesh,
        in_specs=placed,
        out_specs=(P(None, ("groups", "vocab")), P(("groups", "vocab"))),
        check_vma=False,
    )
```

```python
import functools

import jax
import jax.numpy as jnp
from jax import lax
from jax.experimental import pallas as pl
from jax.experimental.pallas import tpu as pltpu
from jax.sharding import PartitionSpec as P

TSN = 1501
SPECIALS = 108
INITIAL = 50

MASK_VALUE = -1000000000.0
EMPTY_VALUE = -3000000000.0
SLOPE = 4.0
FLOOR = -30.0
BIG = 1 << 30
LANES = 128
MESH = pl.DeviceIdType.MESH


def kernel(
    count,
    hidden_ref,
    table_ref,
    prev_ref,
    stamp_ref,
    begin_ref,
    length_ref,
    chosen_ref,
    picked_ref,
    stamp_out_ref,
    rows_all,
    table,
    prev_in,
    stamp_in,
    begin_in,
    length_in,
    chosen_in,
    ordered,
    stats,
    gathered,
    load_sem,
    table_send_sem,
    table_recv_sem,
    send_sem,
    recv_sem,
    stat_send_sem,
    stat_recv_sem,
):
    row_dev = hidden_ref.shape[0]
    width = table_ref.shape[0]
    nsel = chosen_ref.shape[0]
    chips = count // 2
    line = chips // 2
    rows_half = chips * row_dev
    stamp_begin = width * count - TSN
    group = lax.axis_index("groups")
    me = lax.axis_index("vocab")
    chip, core = me // 2, me % 2
    z, x = chip // 2, chip % 2

    def slot(owner):
        return rows_all.at[pl.ds(pl.multiple_of(owner * row_dev, row_dev), row_dev)]

    def half(which):
        return table.at[pl.ds(pl.multiple_of(which * width, width), width)]

    load_own = pltpu.make_async_copy(hidden_ref, slot(chip), load_sem.at[0])
    load_own.start()
    small = [
        pltpu.make_async_copy(source, target, load_sem.at[2 + i])
        for i, (source, target) in enumerate(
            [
                (prev_ref, prev_in),
                (stamp_ref, stamp_in),
                (begin_ref, begin_in),
                (length_ref, length_in),
                (chosen_ref, chosen_in),
            ]
        )
    ]
    for copy in small:
        copy.start()
    load_table = pltpu.make_async_copy(table_ref, half(core), load_sem.at[1])
    load_table.start()

    barrier = pltpu.get_barrier_semaphore()
    for i in range(1, chips):
        pl.semaphore_signal(
            barrier,
            inc=1,
            device_id=(group, ((chip + i) % chips) * 2 + core),
            device_id_type=MESH,
        )
    partner = chip * 2 + 1 - core
    pl.semaphore_signal(barrier, inc=1, device_id=(group, partner), device_id_type=MESH)

    sends = []

    def send(owner, target):
        copy = pltpu.make_async_remote_copy(
            src_ref=slot(owner),
            dst_ref=slot(owner),
            send_sem=send_sem.at[len(sends)],
            recv_sem=recv_sem.at[owner],
            device_id=(group, target * 2 + core),
            device_id_type=MESH,
        )
        copy.start()
        sends.append(copy)

    def arrive(owner):
        pltpu.make_async_remote_copy(
            src_ref=slot(owner),
            dst_ref=slot(owner),
            send_sem=send_sem.at[0],
            recv_sem=recv_sem.at[owner],
            device_id=(group, partner),
            device_id_type=MESH,
        ).wait_recv()

    load_own.wait()
    pl.semaphore_wait(barrier, chips)
    sign = 1 - 2 * ((2 * z) // line)
    across = z * 2 + 1 - x
    order = list(range(line - 1, 0, -1))
    for i in order:
        send(chip, ((z + sign * i + line) % line) * 2 + x)
    send(chip, across)
    share = pltpu.make_async_remote_copy(
        src_ref=table_ref,
        dst_ref=half(core),
        send_sem=table_send_sem,
        recv_sem=table_recv_sem,
        device_id=(group, partner),
        device_id_type=MESH,
    )
    share.start()

    for copy in small:
        copy.wait()
    lane_from = lax.broadcasted_iota(jnp.int32, (2 * LANES, LANES), 0)
    lane_to = lax.broadcasted_iota(jnp.int32, (2 * LANES, LANES), 1)
    wanted = (lane_to // row_dev * 2 + core) * row_dev + lane_to % row_dev
    select = jnp.where(lane_from == wanted, 1.0, 0.0)
    for number in range(rows_half // LANES):
        lanes = pl.ds(number * 2 * LANES, 2 * LANES)
        stacked = jnp.concatenate(
            [
                prev_in[:, lanes],
                stamp_in[:, lanes],
                begin_in[:, lanes],
                length_in[:, lanes],
                chosen_in[:, lanes],
                jnp.zeros((16 - 5 - nsel, 2 * LANES), jnp.int32),
            ],
            axis=0,
        )
        ordered[number] = lax.dot_general(
            stacked.astype(jnp.float32),
            select,
            (((1,), (0,)), ((), ())),
            precision=lax.Precision.HIGHEST,
            preferred_element_type=jnp.float32,
        ).astype(jnp.int32)

    for i in order:
        owner = ((z - sign * i + 2 * line) % line) * 2 + x
        arrive(owner)
        send(owner, across)
    load_table.wait()
    share.wait_recv()
    for i in [0] + order:
        arrive(((z - sign * i + 2 * line) % line) * 2 + 1 - x)

    column = chip * 2 * width + lax.broadcasted_iota(jnp.int32, (2 * width, LANES), 0)
    is_text = column < stamp_begin

    def one_block(number):
        at_row = number * LANES
        if not isinstance(number, int):
            at_row = pl.multiple_of(at_row, LANES)
        logits = lax.dot_general(
            table[...],
            rows_all[pl.ds(at_row, LANES), :],
            (((1,), (1,)), ((), ())),
            preferred_element_type=jnp.float32,
        )
        row = ordered[number]
        generated = row[4:5] - row[3:4]
        last_stamp = row[2:3]
        last_is = (generated >= 1) & (row[1:2] >= stamp_begin)
        before_is = (generated < 2) | (row[0:1] >= stamp_begin)
        opened = last_is & jnp.logical_not(before_is)
        closed = last_is & before_is
        first = generated == 0
        text_low = jnp.where(first, BIG, jnp.where(opened, stamp_begin - SPECIALS, 0))
        bound = last_stamp + jnp.where(opened, 0, 1)
        stamp_low = jnp.where(
            closed, BIG, stamp_begin + jnp.where(last_stamp >= 0, bound, 0)
        )
        stamp_high = jnp.where(first, stamp_begin + INITIAL + 1, BIG)
        low = jnp.where(is_text, text_low, stamp_low)
        high = jnp.where(is_text, stamp_begin - 1, stamp_high)
        values = jnp.where((column >= low) & (column < high), logits, MASK_VALUE)
        text_max = jnp.max(jnp.where(is_text, values, EMPTY_VALUE), axis=0, keepdims=True)
        stamp_max = jnp.max(jnp.where(is_text, EMPTY_VALUE, values), axis=0, keepdims=True)
        powers = jnp.exp(values - jnp.where(is_text, text_max, stamp_max))
        text_total = jnp.sum(jnp.where(is_text, powers, 0.0), axis=0, keepdims=True)
        stamp_total = jnp.sum(jnp.where(is_text, 0.0, powers), axis=0, keepdims=True)
        text_lse = jnp.where(text_total > 0.0, text_max + jnp.log(text_total), EMPTY_VALUE)
        stamp_lse = jnp.where(stamp_total > 0.0, stamp_max + jnp.log(stamp_total), EMPTY_VALUE)
        found = [
            jnp.sum(
                jnp.where(column == row[5 + k : 6 + k], values, 0.0), axis=0, keepdims=True
            )
            for k in range(nsel)
        ]
        lines = [text_max, text_lse, stamp_lse] + found
        lines += [jnp.zeros_like(text_max)] * (8 - len(lines))
        stats[number] = jnp.concatenate(lines, axis=0)

    if rows_half == LANES:
        one_block(0)
    else:
        pl.loop(0, rows_half // LANES)(one_block)

    def stat_copy(i):
        target = (chip + i) % chips
        return pltpu.make_async_remote_copy(
            src_ref=stats.at[(target * row_dev) // LANES],
            dst_ref=gathered.at[chip],
            send_sem=stat_send_sem.at[i],
            recv_sem=stat_recv_sem.at[chip],
            device_id=(group, target * 2 + core),
            device_id_type=MESH,
        )

    stat_sends = [stat_copy(i) for i in range(1, chips)]
    for copy in stat_sends:
        copy.start()
    piece = (chip * row_dev) // LANES
    gathered[chip] = stats[piece]
    for copy in sends:
        copy.wait_send()
    share.wait_send()
    for i in range(1, chips):
        source = (chip + chips - i) % chips
        pltpu.make_async_remote_copy(
            src_ref=stats.at[0],
            dst_ref=gathered.at[source],
            send_sem=stat_send_sem.at[0],
            recv_sem=stat_recv_sem.at[source],
            device_id=(group, partner),
            device_id_type=MESH,
        ).wait_recv()

    tiles = gathered[...]
    top = jnp.max(tiles, axis=0)
    lse = top + jnp.log(jnp.sum(jnp.exp(tiles - top[None]), axis=0))
    picked = jnp.sum(tiles, axis=0)[3 : 3 + nsel]
    text_max, text_lse, stamp_lse = top[0:1], lse[1:2], lse[2:3]
    penalty = SLOPE * jnp.maximum(stamp_lse - text_max, 0.0)
    shifted = text_lse - penalty
    larger = jnp.maximum(shifted, stamp_lse)
    total = larger + jnp.log(jnp.exp(shifted - larger) + jnp.exp(stamp_lse - larger))
    own_chosen = ordered[piece][5 : 5 + nsel]
    adjusted = picked - jnp.where(own_chosen < stamp_begin, penalty, 0.0) - total
    final = jnp.concatenate(
        [adjusted, stamp_lse - total] + [jnp.zeros_like(total)] * (7 - nsel), axis=0
    )
    final = jnp.maximum(final, FLOOR)
    offset = (chip * row_dev) % LANES
    final = pltpu.roll(final, (LANES - offset) % LANES, 1)
    picked_ref[...] = final[:nsel, :row_dev]
    stamp_out_ref[...] = final[nsel : nsel + 1, :row_dev]
    for copy in stat_sends:
        copy.wait_send()


def per_device(hidden, embedding, prev_tokens, last_stamp, sample_begin, seq_length, chosen):
    count = lax.axis_size("vocab")
    row_dev, depth = hidden.shape
    width = embedding.shape[0]
    nsel = chosen.shape[0]
    chips = count // 2
    rows_here = count * row_dev
    rows_half = chips * row_dev
    anywhere = pl.BlockSpec(memory_space=pl.ANY)
    local = pl.BlockSpec(memory_space=pltpu.VMEM)
    picked, stamp = pl.pallas_call(
        functools.partial(kernel, count),
        out_shape=(
            pltpu.VMEM((nsel, row_dev), jnp.float32),
            pltpu.VMEM((1, row_dev), jnp.float32),
        ),
        in_specs=[anywhere] * 7,
        out_specs=(local, local),
        scratch_shapes=[
            pltpu.VMEM((rows_half, depth), hidden.dtype),
            pltpu.VMEM((2 * width, depth), embedding.dtype),
            pltpu.VMEM((2, rows_here), jnp.int32),
            pltpu.VMEM((1, rows_here), jnp.int32),
            pltpu.VMEM((1, rows_here), jnp.int32),
            pltpu.VMEM((1, rows_here), jnp.int32),
            pltpu.VMEM((nsel, rows_here), jnp.int32),
            pltpu.VMEM((rows_half // LANES, 16, LANES), jnp.int32),
            pltpu.VMEM((rows_half // LANES, 8, LANES), jnp.float32),
            pltpu.VMEM((chips, 8, LANES), jnp.float32),
            pltpu.SemaphoreType.DMA((7,)),
            pltpu.SemaphoreType.DMA,
            pltpu.SemaphoreType.DMA,
            pltpu.SemaphoreType.DMA((chips,)),
            pltpu.SemaphoreType.DMA((chips,)),
            pltpu.SemaphoreType.DMA((chips,)),
            pltpu.SemaphoreType.DMA((chips,)),
        ],
        compiler_params=pltpu.CompilerParams(collective_id=0, has_side_effects=True),
        name="decode_step",
    )(
        hidden,
        embedding,
        prev_tokens,
        last_stamp[None, :],
        sample_begin[None, :],
        seq_length[None, :],
        chosen,
    )
    return picked, stamp[0]


def solution(mesh):
    placed = (
        P(("groups", "vocab"), None),
        P("vocab", None),
        P(None, "groups"),
        P("groups"),
        P("groups"),
        P("groups"),
        P(None, "groups"),
    )
    return jax.shard_map(
        per_device,
        mesh=mesh,
        in_specs=placed,
        out_specs=(P(None, ("groups", "vocab")), P(("groups", "vocab"))),
        check_vma=False,
    )
```

```python
import functools

import jax
import jax.numpy as jnp
from jax import lax
from jax.experimental import pallas as pl
from jax.experimental.pallas import tpu as pltpu
from jax.sharding import PartitionSpec as P

TSN = 1501
SPECIALS = 108
INITIAL = 50

MASK_VALUE = -1000000000.0
EMPTY_VALUE = -3000000000.0
SLOPE = 4.0
FLOOR = -30.0
BIG = 1 << 30
LANES = 128
MESH = pl.DeviceIdType.MESH


def kernel(
    count,
    hidden_ref,
    table_ref,
    prev_ref,
    stamp_ref,
    begin_ref,
    length_ref,
    chosen_ref,
    picked_ref,
    stamp_out_ref,
    rows_all,
    table,
    prev_in,
    stamp_in,
    begin_in,
    length_in,
    chosen_in,
    ordered,
    stats,
    gathered,
    load_sem,
    table_send_sem,
    table_recv_sem,
    send_sem,
    recv_sem,
    stat_send_sem,
    stat_recv_sem,
):
    row_dev = hidden_ref.shape[0]
    width = table_ref.shape[0]
    nsel = chosen_ref.shape[0]
    chips = count // 2
    line = chips // 2
    rows_half = chips * row_dev
    stamp_begin = width * count - TSN
    group = lax.axis_index("groups")
    me = lax.axis_index("vocab")
    chip, core = me // 2, me % 2
    z, x = chip // 2, chip % 2

    parts = recv_sem.shape[1]
    cut = rows_all.shape[1] // parts

    def slot(owner, part):
        return rows_all.at[
            pl.ds(pl.multiple_of(owner * row_dev, row_dev), row_dev),
            pl.ds(part * cut, cut),
        ]

    def half(which):
        return table.at[pl.ds(pl.multiple_of(which * width, width), width)]

    load_own = pltpu.make_async_copy(hidden_ref, rows_all.at[pl.ds(pl.multiple_of(chip * row_dev, row_dev), row_dev)], load_sem.at[0])
    load_own.start()
    small = [
        pltpu.make_async_copy(source, target, load_sem.at[2 + i])
        for i, (source, target) in enumerate(
            [
                (prev_ref, prev_in),
                (stamp_ref, stamp_in),
                (begin_ref, begin_in),
                (length_ref, length_in),
                (chosen_ref, chosen_in),
            ]
        )
    ]
    for copy in small:
        copy.start()
    load_table = pltpu.make_async_copy(table_ref, half(core), load_sem.at[1])
    load_table.start()

    barrier = pltpu.get_barrier_semaphore()
    across = z * 2 + 1 - x
    partner = chip * 2 + 1 - core
    greeted = [(((z + i) % line) * 2 + x) * 2 + core for i in range(1, line)]
    greeted += [across * 2 + core, partner]
    for peer in greeted:
        pl.semaphore_signal(barrier, inc=1, device_id=(group, peer), device_id_type=MESH)

    sends = []

    def send(owner, part, target):
        copy = pltpu.make_async_remote_copy(
            src_ref=slot(owner, part),
            dst_ref=slot(owner, part),
            send_sem=send_sem.at[len(sends)],
            recv_sem=recv_sem.at[owner, part],
            device_id=(group, target * 2 + core),
            device_id_type=MESH,
        )
        copy.start()
        sends.append(copy)

    def arrive(owner, part):
        pltpu.make_async_remote_copy(
            src_ref=slot(owner, part),
            dst_ref=slot(owner, part),
            send_sem=send_sem.at[0],
            recv_sem=recv_sem.at[owner, part],
            device_id=(group, partner),
            device_id_type=MESH,
        ).wait_recv()

    load_own.wait()
    pl.semaphore_wait(barrier, len(greeted))
    sign = 1 - 2 * ((2 * z) // line)
    order = list(range(line - 1, 0, -1))
    for part in range(parts):
        for i in order:
            send(chip, part, ((z + sign * i + line) % line) * 2 + x)
        send(chip, part, across)
    share = pltpu.make_async_remote_copy(
        src_ref=table_ref,
        dst_ref=half(core),
        send_sem=table_send_sem,
        recv_sem=table_recv_sem,
        device_id=(group, partner),
        device_id_type=MESH,
    )
    share.start()

    for copy in small:
        copy.wait()
    lane_from = lax.broadcasted_iota(jnp.int32, (2 * LANES, LANES), 0)
    lane_to = lax.broadcasted_iota(jnp.int32, (2 * LANES, LANES), 1)
    wanted = (lane_to // row_dev * 2 + core) * row_dev + lane_to % row_dev
    select = jnp.where(lane_from == wanted, 1.0, 0.0)
    for number in range(rows_half // LANES):
        lanes = pl.ds(number * 2 * LANES, 2 * LANES)
        stacked = jnp.concatenate(
            [
                prev_in[:, lanes],
                stamp_in[:, lanes],
                begin_in[:, lanes],
                length_in[:, lanes],
                chosen_in[:, lanes],
                jnp.zeros((16 - 5 - nsel, 2 * LANES), jnp.int32),
            ],
            axis=0,
        )
        ordered[number] = lax.dot_general(
            stacked.astype(jnp.float32),
            select,
            (((1,), (0,)), ((), ())),
            precision=lax.Precision.HIGHEST,
            preferred_element_type=jnp.float32,
        ).astype(jnp.int32)

    for part in range(parts):
        for i in order:
            owner = ((z - sign * i + 2 * line) % line) * 2 + x
            arrive(owner, part)
            send(owner, part, across)
    load_table.wait()
    share.wait_recv()
    for part in range(parts):
        for i in [0] + order:
            arrive(((z - sign * i + 2 * line) % line) * 2 + 1 - x, part)

    column = chip * 2 * width + lax.broadcasted_iota(jnp.int32, (2 * width, LANES), 0)
    is_text = column < stamp_begin

    def one_block(number):
        at_row = number * LANES
        if not isinstance(number, int):
            at_row = pl.multiple_of(at_row, LANES)
        logits = lax.dot_general(
            table[...],
            rows_all[pl.ds(at_row, LANES), :],
            (((1,), (1,)), ((), ())),
            preferred_element_type=jnp.float32,
        )
        row = ordered[number]
        generated = row[4:5] - row[3:4]
        last_stamp = row[2:3]
        last_is = (generated >= 1) & (row[1:2] >= stamp_begin)
        before_is = (generated < 2) | (row[0:1] >= stamp_begin)
        opened = last_is & jnp.logical_not(before_is)
        closed = last_is & before_is
        first = generated == 0
        text_low = jnp.where(first, BIG, jnp.where(opened, stamp_begin - SPECIALS, 0))
        bound = last_stamp + jnp.where(opened, 0, 1)
        stamp_low = jnp.where(
            closed, BIG, stamp_begin + jnp.where(last_stamp >= 0, bound, 0)
        )
        stamp_high = jnp.where(first, stamp_begin + INITIAL + 1, BIG)
        low = jnp.where(is_text, text_low, stamp_low)
        high = jnp.where(is_text, stamp_begin - 1, stamp_high)
        values = jnp.where((column >= low) & (column < high), logits, MASK_VALUE)
        text_max = jnp.max(jnp.where(is_text, values, EMPTY_VALUE), axis=0, keepdims=True)
        stamp_max = jnp.max(jnp.where(is_text, EMPTY_VALUE, values), axis=0, keepdims=True)
        powers = jnp.exp(values - jnp.where(is_text, text_max, stamp_max))
        text_total = jnp.sum(jnp.where(is_text, powers, 0.0), axis=0, keepdims=True)
        stamp_total = jnp.sum(jnp.where(is_text, 0.0, powers), axis=0, keepdims=True)
        text_lse = jnp.where(text_total > 0.0, text_max + jnp.log(text_total), EMPTY_VALUE)
        stamp_lse = jnp.where(stamp_total > 0.0, stamp_max + jnp.log(stamp_total), EMPTY_VALUE)
        found = [
            jnp.sum(
                jnp.where(column == row[5 + k : 6 + k], values, 0.0), axis=0, keepdims=True
            )
            for k in range(nsel)
        ]
        lines = [text_max, text_lse, stamp_lse] + found
        lines += [jnp.zeros_like(text_max)] * (8 - len(lines))
        stats[number] = jnp.concatenate(lines, axis=0)

    if rows_half == LANES:
        one_block(0)
    else:
        pl.loop(0, rows_half // LANES)(one_block)

    def stat_copy(i):
        target = (chip + sign * i + chips) % chips
        return pltpu.make_async_remote_copy(
            src_ref=stats.at[(target * row_dev) // LANES],
            dst_ref=gathered.at[chip],
            send_sem=stat_send_sem.at[i],
            recv_sem=stat_recv_sem.at[chip],
            device_id=(group, target * 2 + core),
            device_id_type=MESH,
        )

    stat_sends = [stat_copy(i) for i in range(chips - 1, 0, -1)]
    for copy in stat_sends:
        copy.start()
    piece = (chip * row_dev) // LANES
    gathered[chip] = stats[piece]
    for copy in sends:
        copy.wait_send()
    share.wait_send()
    for i in range(1, chips):
        source = (chip + chips - i) % chips
        pltpu.make_async_remote_copy(
            src_ref=stats.at[0],
            dst_ref=gathered.at[source],
            send_sem=stat_send_sem.at[0],
            recv_sem=stat_recv_sem.at[source],
            device_id=(group, partner),
            device_id_type=MESH,
        ).wait_recv()

    tiles = gathered[...]
    top = jnp.max(tiles, axis=0)
    lse = top + jnp.log(jnp.sum(jnp.exp(tiles - top[None]), axis=0))
    picked = jnp.sum(tiles, axis=0)[3 : 3 + nsel]
    text_max, text_lse, stamp_lse = top[0:1], lse[1:2], lse[2:3]
    penalty = SLOPE * jnp.maximum(stamp_lse - text_max, 0.0)
    shifted = text_lse - penalty
    larger = jnp.maximum(shifted, stamp_lse)
    total = larger + jnp.log(jnp.exp(shifted - larger) + jnp.exp(stamp_lse - larger))
    own_chosen = ordered[piece][5 : 5 + nsel]
    adjusted = picked - jnp.where(own_chosen < stamp_begin, penalty, 0.0) - total
    final = jnp.concatenate(
        [adjusted, stamp_lse - total] + [jnp.zeros_like(total)] * (7 - nsel), axis=0
    )
    final = jnp.maximum(final, FLOOR)
    offset = (chip * row_dev) % LANES
    final = pltpu.roll(final, (LANES - offset) % LANES, 1)
    picked_ref[...] = final[:nsel, :row_dev]
    stamp_out_ref[...] = final[nsel : nsel + 1, :row_dev]
    for copy in stat_sends:
        copy.wait_send()


def per_device(hidden, embedding, prev_tokens, last_stamp, sample_begin, seq_length, chosen):
    count = lax.axis_size("vocab")
    row_dev, depth = hidden.shape
    width = embedding.shape[0]
    nsel = chosen.shape[0]
    chips = count // 2
    rows_here = count * row_dev
    rows_half = chips * row_dev
    parts = 2 if depth % (2 * LANES) == 0 else 1
    anywhere = pl.BlockSpec(memory_space=pl.ANY)
    local = pl.BlockSpec(memory_space=pltpu.VMEM)
    picked, stamp = pl.pallas_call(
        functools.partial(kernel, count),
        out_shape=(
            pltpu.VMEM((nsel, row_dev), jnp.float32),
            pltpu.VMEM((1, row_dev), jnp.float32),
        ),
        in_specs=[anywhere] * 7,
        out_specs=(local, local),
        scratch_shapes=[
            pltpu.VMEM((rows_half, depth), hidden.dtype),
            pltpu.VMEM((2 * width, depth), embedding.dtype),
            pltpu.VMEM((2, rows_here), jnp.int32),
            pltpu.VMEM((1, rows_here), jnp.int32),
            pltpu.VMEM((1, rows_here), jnp.int32),
            pltpu.VMEM((1, rows_here), jnp.int32),
            pltpu.VMEM((nsel, rows_here), jnp.int32),
            pltpu.VMEM((rows_half // LANES, 16, LANES), jnp.int32),
            pltpu.VMEM((rows_half // LANES, 8, LANES), jnp.float32),
            pltpu.VMEM((chips, 8, LANES), jnp.float32),
            pltpu.SemaphoreType.DMA((7,)),
            pltpu.SemaphoreType.DMA,
            pltpu.SemaphoreType.DMA,
            pltpu.SemaphoreType.DMA((chips * parts,)),
            pltpu.SemaphoreType.DMA((chips, parts)),
            pltpu.SemaphoreType.DMA((chips,)),
            pltpu.SemaphoreType.DMA((chips,)),
        ],
        compiler_params=pltpu.CompilerParams(collective_id=0, has_side_effects=True),
        name="decode_step",
    )(
        hidden,
        embedding,
        prev_tokens,
        last_stamp[None, :],
        sample_begin[None, :],
        seq_length[None, :],
        chosen,
    )
    return picked, stamp[0]


def solution(mesh):
    placed = (
        P(("groups", "vocab"), None),
        P("vocab", None),
        P(None, "groups"),
        P("groups"),
        P("groups"),
        P("groups"),
        P(None, "groups"),
    )
    return jax.shard_map(
        per_device,
        mesh=mesh,
        in_specs=placed,
        out_specs=(P(None, ("groups", "vocab")), P(("groups", "vocab"))),
        check_vma=False,
    )
```

```python
import functools

import jax
import jax.numpy as jnp
from jax import lax
from jax.experimental import pallas as pl
from jax.experimental.pallas import tpu as pltpu
from jax.sharding import PartitionSpec as P

TSN = 1501
SPECIALS = 108
INITIAL = 50

MASK_VALUE = -1000000000.0
EMPTY_VALUE = -3000000000.0
SLOPE = 4.0
FLOOR = -30.0
BIG = 1 << 30
LANES = 128
MESH = pl.DeviceIdType.MESH


def kernel(
    count,
    hidden_ref,
    table_ref,
    prev_ref,
    stamp_ref,
    begin_ref,
    length_ref,
    chosen_ref,
    picked_ref,
    stamp_out_ref,
    rows_all,
    table,
    prev_in,
    stamp_in,
    begin_in,
    length_in,
    chosen_in,
    ordered,
    partial,
    stats,
    gathered,
    load_sem,
    table_send_sem,
    table_recv_sem,
    send_sem,
    recv_sem,
    stat_send_sem,
    stat_recv_sem,
):
    row_dev = hidden_ref.shape[0]
    width = table_ref.shape[0]
    nsel = chosen_ref.shape[0]
    chips = count // 2
    line = chips // 2
    rows_half = chips * row_dev
    stamp_begin = width * count - TSN
    group = lax.axis_index("groups")
    me = lax.axis_index("vocab")
    chip, core = me // 2, me % 2
    z, x = chip // 2, chip % 2

    parts = recv_sem.shape[1]
    cut = rows_all.shape[1] // parts

    def slot(owner, part):
        return rows_all.at[
            pl.ds(pl.multiple_of(owner * row_dev, row_dev), row_dev),
            pl.ds(part * cut, cut),
        ]

    def half(which):
        return table.at[pl.ds(pl.multiple_of(which * width, width), width)]

    load_own = pltpu.make_async_copy(hidden_ref, rows_all.at[pl.ds(pl.multiple_of(chip * row_dev, row_dev), row_dev)], load_sem.at[0])
    load_own.start()

    barrier = pltpu.get_barrier_semaphore()
    across = z * 2 + 1 - x
    partner = chip * 2 + 1 - core
    greeted = [(((z + i) % line) * 2 + x) * 2 + core for i in range(1, line)]
    greeted += [across * 2 + core, partner]
    for peer in greeted:
        pl.semaphore_signal(barrier, inc=1, device_id=(group, peer), device_id_type=MESH)
    small = [
        pltpu.make_async_copy(source, target, load_sem.at[2 + i])
        for i, (source, target) in enumerate(
            [
                (prev_ref, prev_in),
                (stamp_ref, stamp_in),
                (begin_ref, begin_in),
                (length_ref, length_in),
                (chosen_ref, chosen_in),
            ]
        )
    ]
    for copy in small:
        copy.start()
    load_table = pltpu.make_async_copy(table_ref, half(core), load_sem.at[1])
    load_table.start()

    sends = []

    def send(owner, part, target):
        copy = pltpu.make_async_remote_copy(
            src_ref=slot(owner, part),
            dst_ref=slot(owner, part),
            send_sem=send_sem.at[len(sends)],
            recv_sem=recv_sem.at[owner, part],
            device_id=(group, target * 2 + core),
            device_id_type=MESH,
        )
        copy.start()
        sends.append(copy)

    def arrive(owner, part):
        pltpu.make_async_remote_copy(
            src_ref=slot(owner, part),
            dst_ref=slot(owner, part),
            send_sem=send_sem.at[0],
            recv_sem=recv_sem.at[owner, part],
            device_id=(group, partner),
            device_id_type=MESH,
        ).wait_recv()

    load_own.wait()
    pl.semaphore_wait(barrier, len(greeted))
    sign = 1 - 2 * ((2 * z) // line)
    order = list(range(line - 1, 0, -1))
    for part in range(parts):
        for i in order:
            send(chip, part, ((z + sign * i + line) % line) * 2 + x)
        send(chip, part, across)
    share = pltpu.make_async_remote_copy(
        src_ref=table_ref,
        dst_ref=half(core),
        send_sem=table_send_sem,
        recv_sem=table_recv_sem,
        device_id=(group, partner),
        device_id_type=MESH,
    )
    share.start()

    for copy in small:
        copy.wait()
    lane_from = lax.broadcasted_iota(jnp.int32, (2 * LANES, LANES), 0)
    lane_to = lax.broadcasted_iota(jnp.int32, (2 * LANES, LANES), 1)
    wanted = (lane_to // row_dev * 2 + core) * row_dev + lane_to % row_dev
    select = jnp.where(lane_from == wanted, 1.0, 0.0)
    for number in range(rows_half // LANES):
        lanes = pl.ds(number * 2 * LANES, 2 * LANES)
        stacked = jnp.concatenate(
            [
                prev_in[:, lanes],
                stamp_in[:, lanes],
                begin_in[:, lanes],
                length_in[:, lanes],
                chosen_in[:, lanes],
                jnp.zeros((16 - 5 - nsel, 2 * LANES), jnp.int32),
            ],
            axis=0,
        )
        ordered[number] = lax.dot_general(
            stacked.astype(jnp.float32),
            select,
            (((1,), (0,)), ((), ())),
            precision=lax.Precision.HIGHEST,
            preferred_element_type=jnp.float32,
        ).astype(jnp.int32)

    for part in range(parts):
        for i in order:
            owner = ((z - sign * i + 2 * line) % line) * 2 + x
            arrive(owner, part)
            send(owner, part, across)
    load_table.wait()
    share.wait_recv()

    def multiply(number, part):
        at_row = number * LANES
        if not isinstance(number, int):
            at_row = pl.multiple_of(at_row, LANES)
        product = lax.dot_general(
            table[:, part * cut : (part + 1) * cut],
            rows_all[pl.ds(at_row, LANES), part * cut : (part + 1) * cut],
            (((1,), (1,)), ((), ())),
            preferred_element_type=jnp.float32,
        )
        return product if part == 0 else product + partial[number]

    for part in range(parts):
        for i in [0] + order:
            arrive(((z - sign * i + 2 * line) % line) * 2 + 1 - x, part)
        if part < parts - 1:

            def add_part(number, part=part):
                partial[number] = multiply(number, part)

            if rows_half == LANES:
                add_part(0)
            else:
                pl.loop(0, rows_half // LANES)(add_part)

    column = chip * 2 * width + lax.broadcasted_iota(jnp.int32, (2 * width, LANES), 0)
    is_text = column < stamp_begin

    def one_block(number):
        logits = multiply(number, parts - 1)
        row = ordered[number]
        generated = row[4:5] - row[3:4]
        last_stamp = row[2:3]
        last_is = (generated >= 1) & (row[1:2] >= stamp_begin)
        before_is = (generated < 2) | (row[0:1] >= stamp_begin)
        opened = last_is & jnp.logical_not(before_is)
        closed = last_is & before_is
        first = generated == 0
        text_low = jnp.where(first, BIG, jnp.where(opened, stamp_begin - SPECIALS, 0))
        bound = last_stamp + jnp.where(opened, 0, 1)
        stamp_low = jnp.where(
            closed, BIG, stamp_begin + jnp.where(last_stamp >= 0, bound, 0)
        )
        stamp_high = jnp.where(first, stamp_begin + INITIAL + 1, BIG)
        low = jnp.where(is_text, text_low, stamp_low)
        high = jnp.where(is_text, stamp_begin - 1, stamp_high)
        values = jnp.where((column >= low) & (column < high), logits, MASK_VALUE)
        text_max = jnp.max(jnp.where(is_text, values, EMPTY_VALUE), axis=0, keepdims=True)
        stamp_max = jnp.max(jnp.where(is_text, EMPTY_VALUE, values), axis=0, keepdims=True)
        powers = jnp.exp(values - jnp.where(is_text, text_max, stamp_max))
        text_total = jnp.sum(jnp.where(is_text, powers, 0.0), axis=0, keepdims=True)
        stamp_total = jnp.sum(jnp.where(is_text, 0.0, powers), axis=0, keepdims=True)
        text_lse = jnp.where(text_total > 0.0, text_max + jnp.log(text_total), EMPTY_VALUE)
        stamp_lse = jnp.where(stamp_total > 0.0, stamp_max + jnp.log(stamp_total), EMPTY_VALUE)
        found = [
            jnp.sum(
                jnp.where(column == row[5 + k : 6 + k], values, 0.0), axis=0, keepdims=True
            )
            for k in range(nsel)
        ]
        lines = [text_max, text_lse, stamp_lse] + found
        lines += [jnp.zeros_like(text_max)] * (8 - len(lines))
        stats[number] = jnp.concatenate(lines, axis=0)

    if rows_half == LANES:
        one_block(0)
    else:
        pl.loop(0, rows_half // LANES)(one_block)

    def stat_copy(i):
        target = (chip + sign * i + chips) % chips
        return pltpu.make_async_remote_copy(
            src_ref=stats.at[(target * row_dev) // LANES],
            dst_ref=gathered.at[chip],
            send_sem=stat_send_sem.at[i],
            recv_sem=stat_recv_sem.at[chip],
            device_id=(group, target * 2 + core),
            device_id_type=MESH,
        )

    stat_sends = [stat_copy(i) for i in range(chips - 1, 0, -1)]
    for copy in stat_sends:
        copy.start()
    piece = (chip * row_dev) // LANES
    gathered[chip] = stats[piece]
    for copy in sends:
        copy.wait_send()
    share.wait_send()
    for i in range(1, chips):
        source = (chip + chips - i) % chips
        pltpu.make_async_remote_copy(
            src_ref=stats.at[0],
            dst_ref=gathered.at[source],
            send_sem=stat_send_sem.at[0],
            recv_sem=stat_recv_sem.at[source],
            device_id=(group, partner),
            device_id_type=MESH,
        ).wait_recv()

    tiles = gathered[...]
    top = jnp.max(tiles, axis=0)
    lse = top + jnp.log(jnp.sum(jnp.exp(tiles - top[None]), axis=0))
    picked = jnp.sum(tiles, axis=0)[3 : 3 + nsel]
    text_max, text_lse, stamp_lse = top[0:1], lse[1:2], lse[2:3]
    penalty = SLOPE * jnp.maximum(stamp_lse - text_max, 0.0)
    shifted = text_lse - penalty
    larger = jnp.maximum(shifted, stamp_lse)
    total = larger + jnp.log(jnp.exp(shifted - larger) + jnp.exp(stamp_lse - larger))
    own_chosen = ordered[piece][5 : 5 + nsel]
    adjusted = picked - jnp.where(own_chosen < stamp_begin, penalty, 0.0) - total
    final = jnp.concatenate(
        [adjusted, stamp_lse - total] + [jnp.zeros_like(total)] * (7 - nsel), axis=0
    )
    final = jnp.maximum(final, FLOOR)
    offset = (chip * row_dev) % LANES
    final = pltpu.roll(final, (LANES - offset) % LANES, 1)
    picked_ref[...] = final[:nsel, :row_dev]
    stamp_out_ref[...] = final[nsel : nsel + 1, :row_dev]
    for copy in stat_sends:
        copy.wait_send()


def emit(picked_ref, stamp_ref, picked_out, stamp_out, sem):
    first = pltpu.make_async_copy(picked_ref, picked_out, sem.at[0])
    second = pltpu.make_async_copy(stamp_ref, stamp_out, sem.at[1])
    first.start()
    second.start()
    first.wait()
    second.wait()


def per_device(hidden, embedding, prev_tokens, last_stamp, sample_begin, seq_length, chosen):
    count = lax.axis_size("vocab")
    row_dev, depth = hidden.shape
    width = embedding.shape[0]
    nsel = chosen.shape[0]
    chips = count // 2
    rows_here = count * row_dev
    rows_half = chips * row_dev
    parts = 2 if depth % (2 * LANES) == 0 else 1
    anywhere = pl.BlockSpec(memory_space=pl.ANY)
    local = pl.BlockSpec(memory_space=pltpu.VMEM)
    picked, stamp = pl.pallas_call(
        functools.partial(kernel, count),
        out_shape=(
            pltpu.VMEM((nsel, row_dev), jnp.float32),
            pltpu.VMEM((1, row_dev), jnp.float32),
        ),
        in_specs=[anywhere] * 7,
        out_specs=(local, local),
        scratch_shapes=[
            pltpu.VMEM((rows_half, depth), hidden.dtype),
            pltpu.VMEM((2 * width, depth), embedding.dtype),
            pltpu.VMEM((2, rows_here), jnp.int32),
            pltpu.VMEM((1, rows_here), jnp.int32),
            pltpu.VMEM((1, rows_here), jnp.int32),
            pltpu.VMEM((1, rows_here), jnp.int32),
            pltpu.VMEM((nsel, rows_here), jnp.int32),
            pltpu.VMEM((rows_half // LANES, 16, LANES), jnp.int32),
            pltpu.VMEM((rows_half // LANES, 2 * width, LANES), jnp.float32),
            pltpu.VMEM((rows_half // LANES, 8, LANES), jnp.float32),
            pltpu.VMEM((chips, 8, LANES), jnp.float32),
            pltpu.SemaphoreType.DMA((7,)),
            pltpu.SemaphoreType.DMA,
            pltpu.SemaphoreType.DMA,
            pltpu.SemaphoreType.DMA((chips * parts,)),
            pltpu.SemaphoreType.DMA((chips, parts)),
            pltpu.SemaphoreType.DMA((chips,)),
            pltpu.SemaphoreType.DMA((chips,)),
        ],
        compiler_params=pltpu.CompilerParams(collective_id=0, has_side_effects=True),
        name="decode_step",
    )(
        hidden,
        embedding,
        prev_tokens,
        last_stamp[None, :],
        sample_begin[None, :],
        seq_length[None, :],
        chosen,
    )
    picked, stamp = pl.pallas_call(
        emit,
        out_shape=(
            jax.ShapeDtypeStruct((nsel, row_dev), jnp.float32),
            jax.ShapeDtypeStruct((1, row_dev), jnp.float32),
        ),
        in_specs=[local, local],
        out_specs=(anywhere, anywhere),
        scratch_shapes=[pltpu.SemaphoreType.DMA((2,))],
        name="emit",
    )(
        pltpu.with_memory_space_constraint(picked, pltpu.VMEM),
        pltpu.with_memory_space_constraint(stamp, pltpu.VMEM),
    )
    return picked, stamp[0]


def solution(mesh):
    placed = (
        P(("groups", "vocab"), None),
        P("vocab", None),
        P(None, "groups"),
        P("groups"),
        P("groups"),
        P("groups"),
        P(None, "groups"),
    )
    return jax.shard_map(
        per_device,
        mesh=mesh,
        in_specs=placed,
        out_specs=(P(None, ("groups", "vocab")), P(("groups", "vocab"))),
        check_vma=False,
    )
```

```python
import functools

import jax
import jax.numpy as jnp
from jax import lax
from jax.experimental import pallas as pl
from jax.experimental.pallas import tpu as pltpu
from jax.sharding import PartitionSpec as P

TSN = 1501
SPECIALS = 108
INITIAL = 50

MASK_VALUE = -1000000000.0
EMPTY_VALUE = -3000000000.0
SLOPE = 4.0
FLOOR = -30.0
BIG = 1 << 30
LANES = 128
MESH = pl.DeviceIdType.MESH


def kernel(
    count,
    hidden_ref,
    table_ref,
    prev_ref,
    stamp_ref,
    begin_ref,
    length_ref,
    chosen_ref,
    picked_ref,
    stamp_out_ref,
    rows_all,
    table,
    prev_in,
    stamp_in,
    begin_in,
    length_in,
    chosen_in,
    ordered,
    partial,
    kept,
    stats,
    gathered,
    load_sem,
    table_send_sem,
    table_recv_sem,
    send_sem,
    recv_sem,
    stat_send_sem,
    stat_recv_sem,
):
    row_dev = hidden_ref.shape[0]
    width = table_ref.shape[0]
    nsel = chosen_ref.shape[0]
    chips = count // 2
    line = chips // 2
    rows_half = chips * row_dev
    stamp_begin = width * count - TSN
    group = lax.axis_index("groups")
    me = lax.axis_index("vocab")
    chip, core = me // 2, me % 2
    z, x = chip // 2, chip % 2

    parts = recv_sem.shape[1]
    cut = rows_all.shape[1] // parts

    def slot(owner, part):
        return rows_all.at[
            pl.ds(pl.multiple_of(owner * row_dev, row_dev), row_dev),
            pl.ds(part * cut, cut),
        ]

    def half(which):
        return table.at[pl.ds(pl.multiple_of(which * width, width), width)]

    load_own = pltpu.make_async_copy(hidden_ref, rows_all.at[pl.ds(pl.multiple_of(chip * row_dev, row_dev), row_dev)], load_sem.at[0])
    load_own.start()

    barrier = pltpu.get_barrier_semaphore()
    across = z * 2 + 1 - x
    partner = chip * 2 + 1 - core
    greeted = [(((z + i) % line) * 2 + x) * 2 + core for i in range(1, line)]
    greeted += [across * 2 + core, partner]
    for peer in greeted:
        pl.semaphore_signal(barrier, inc=1, device_id=(group, peer), device_id_type=MESH)
    small = [
        pltpu.make_async_copy(source, target, load_sem.at[2 + i])
        for i, (source, target) in enumerate(
            [
                (prev_ref, prev_in),
                (stamp_ref, stamp_in),
                (begin_ref, begin_in),
                (length_ref, length_in),
                (chosen_ref, chosen_in),
            ]
        )
    ]
    for copy in small:
        copy.start()
    load_table = pltpu.make_async_copy(table_ref, half(core), load_sem.at[1])
    load_table.start()

    sends = []

    def send(owner, part, target):
        copy = pltpu.make_async_remote_copy(
            src_ref=slot(owner, part),
            dst_ref=slot(owner, part),
            send_sem=send_sem.at[len(sends)],
            recv_sem=recv_sem.at[owner, part],
            device_id=(group, target * 2 + core),
            device_id_type=MESH,
        )
        copy.start()
        sends.append(copy)

    def arrive(owner, part):
        pltpu.make_async_remote_copy(
            src_ref=slot(owner, part),
            dst_ref=slot(owner, part),
            send_sem=send_sem.at[0],
            recv_sem=recv_sem.at[owner, part],
            device_id=(group, partner),
            device_id_type=MESH,
        ).wait_recv()

    load_own.wait()
    pl.semaphore_wait(barrier, len(greeted))
    sign = 1 - 2 * ((2 * z) // line)
    order = list(range(line - 1, 0, -1))
    for part in range(parts):
        for i in order:
            send(chip, part, ((z + sign * i + line) % line) * 2 + x)
        send(chip, part, across)
    share = pltpu.make_async_remote_copy(
        src_ref=table_ref,
        dst_ref=half(core),
        send_sem=table_send_sem,
        recv_sem=table_recv_sem,
        device_id=(group, partner),
        device_id_type=MESH,
    )
    share.start()

    for copy in small:
        copy.wait()
    lane_from = lax.broadcasted_iota(jnp.int32, (2 * LANES, LANES), 0)
    lane_to = lax.broadcasted_iota(jnp.int32, (2 * LANES, LANES), 1)
    wanted = (lane_to // row_dev * 2 + core) * row_dev + lane_to % row_dev
    select = jnp.where(lane_from == wanted, 1.0, 0.0)
    for number in range(rows_half // LANES):
        lanes = pl.ds(number * 2 * LANES, 2 * LANES)
        stacked = jnp.concatenate(
            [
                prev_in[:, lanes],
                stamp_in[:, lanes],
                begin_in[:, lanes],
                length_in[:, lanes],
                chosen_in[:, lanes],
                jnp.zeros((16 - 5 - nsel, 2 * LANES), jnp.int32),
            ],
            axis=0,
        )
        ordered[number] = lax.dot_general(
            stacked.astype(jnp.float32),
            select,
            (((1,), (0,)), ((), ())),
            precision=lax.Precision.HIGHEST,
            preferred_element_type=jnp.float32,
        ).astype(jnp.int32)

    for part in range(parts):
        for i in order:
            owner = ((z - sign * i + 2 * line) % line) * 2 + x
            arrive(owner, part)
            send(owner, part, across)
    load_table.wait()
    share.wait_recv()

    column = chip * 2 * width + lax.broadcasted_iota(jnp.int32, (2 * width, LANES), 0)
    is_text = column < stamp_begin

    for number in range(rows_half // LANES):
        row = ordered[number]
        generated = row[4:5] - row[3:4]
        last_stamp = row[2:3]
        last_is = (generated >= 1) & (row[1:2] >= stamp_begin)
        before_is = (generated < 2) | (row[0:1] >= stamp_begin)
        opened = last_is & jnp.logical_not(before_is)
        closed = last_is & before_is
        first = generated == 0
        text_low = jnp.where(first, BIG, jnp.where(opened, stamp_begin - SPECIALS, 0))
        bound = last_stamp + jnp.where(opened, 0, 1)
        stamp_low = jnp.where(
            closed, BIG, stamp_begin + jnp.where(last_stamp >= 0, bound, 0)
        )
        stamp_high = jnp.where(first, stamp_begin + INITIAL + 1, BIG)
        low = jnp.where(is_text, text_low, stamp_low)
        high = jnp.where(is_text, stamp_begin - 1, stamp_high)
        kept[number] = jnp.where((column >= low) & (column < high), 1.0, 0.0)

    def multiply(number, part):
        at_row = number * LANES
        if not isinstance(number, int):
            at_row = pl.multiple_of(at_row, LANES)
        product = lax.dot_general(
            table[:, part * cut : (part + 1) * cut],
            rows_all[pl.ds(at_row, LANES), part * cut : (part + 1) * cut],
            (((1,), (1,)), ((), ())),
            preferred_element_type=jnp.float32,
        )
        return product if part == 0 else product + partial[number]

    for part in range(parts):
        for i in [0] + order:
            arrive(((z - sign * i + 2 * line) % line) * 2 + 1 - x, part)
        if part < parts - 1:

            def add_part(number, part=part):
                partial[number] = multiply(number, part)

            if rows_half == LANES:
                add_part(0)
            else:
                pl.loop(0, rows_half // LANES)(add_part)

    def one_block(number):
        logits = multiply(number, parts - 1)
        row = ordered[number]
        values = jnp.where(kept[number] > 0.0, logits, MASK_VALUE)
        text_max = jnp.max(jnp.where(is_text, values, EMPTY_VALUE), axis=0, keepdims=True)
        stamp_max = jnp.max(jnp.where(is_text, EMPTY_VALUE, values), axis=0, keepdims=True)
        powers = jnp.exp(values - jnp.where(is_text, text_max, stamp_max))
        text_total = jnp.sum(jnp.where(is_text, powers, 0.0), axis=0, keepdims=True)
        stamp_total = jnp.sum(jnp.where(is_text, 0.0, powers), axis=0, keepdims=True)
        text_lse = jnp.where(text_total > 0.0, text_max + jnp.log(text_total), EMPTY_VALUE)
        stamp_lse = jnp.where(stamp_total > 0.0, stamp_max + jnp.log(stamp_total), EMPTY_VALUE)
        found = [
            jnp.sum(
                jnp.where(column == row[5 + k : 6 + k], values, 0.0), axis=0, keepdims=True
            )
            for k in range(nsel)
        ]
        lines = [text_max, text_lse, stamp_lse] + found
        lines += [jnp.zeros_like(text_max)] * (8 - len(lines))
        stats[number] = jnp.concatenate(lines, axis=0)

    if rows_half == LANES:
        one_block(0)
    else:
        pl.loop(0, rows_half // LANES)(one_block)

    def stat_copy(i):
        target = (chip + sign * i + chips) % chips
        return pltpu.make_async_remote_copy(
            src_ref=stats.at[(target * row_dev) // LANES],
            dst_ref=gathered.at[chip],
            send_sem=stat_send_sem.at[i],
            recv_sem=stat_recv_sem.at[chip],
            device_id=(group, target * 2 + core),
            device_id_type=MESH,
        )

    stat_sends = [stat_copy(i) for i in range(chips - 1, 0, -1)]
    for copy in stat_sends:
        copy.start()
    piece = (chip * row_dev) // LANES
    gathered[chip] = stats[piece]
    for copy in sends:
        copy.wait_send()
    share.wait_send()
    for i in range(1, chips):
        source = (chip + chips - i) % chips
        pltpu.make_async_remote_copy(
            src_ref=stats.at[0],
            dst_ref=gathered.at[source],
            send_sem=stat_send_sem.at[0],
            recv_sem=stat_recv_sem.at[source],
            device_id=(group, partner),
            device_id_type=MESH,
        ).wait_recv()

    tiles = gathered[...]
    top = jnp.max(tiles, axis=0)
    lse = top + jnp.log(jnp.sum(jnp.exp(tiles - top[None]), axis=0))
    picked = jnp.sum(tiles, axis=0)[3 : 3 + nsel]
    text_max, text_lse, stamp_lse = top[0:1], lse[1:2], lse[2:3]
    penalty = SLOPE * jnp.maximum(stamp_lse - text_max, 0.0)
    shifted = text_lse - penalty
    larger = jnp.maximum(shifted, stamp_lse)
    total = larger + jnp.log(jnp.exp(shifted - larger) + jnp.exp(stamp_lse - larger))
    own_chosen = ordered[piece][5 : 5 + nsel]
    adjusted = picked - jnp.where(own_chosen < stamp_begin, penalty, 0.0) - total
    final = jnp.concatenate(
        [adjusted, stamp_lse - total] + [jnp.zeros_like(total)] * (7 - nsel), axis=0
    )
    final = jnp.maximum(final, FLOOR)
    offset = (chip * row_dev) % LANES
    final = pltpu.roll(final, (LANES - offset) % LANES, 1)
    picked_ref[...] = final[:nsel, :row_dev]
    stamp_out_ref[...] = final[nsel : nsel + 1, :row_dev]
    for copy in stat_sends:
        copy.wait_send()


def emit(picked_ref, stamp_ref, picked_out, stamp_out, sem):
    first = pltpu.make_async_copy(picked_ref, picked_out, sem.at[0])
    second = pltpu.make_async_copy(stamp_ref, stamp_out, sem.at[1])
    first.start()
    second.start()
    first.wait()
    second.wait()


def per_device(hidden, embedding, prev_tokens, last_stamp, sample_begin, seq_length, chosen):
    count = lax.axis_size("vocab")
    row_dev, depth = hidden.shape
    width = embedding.shape[0]
    nsel = chosen.shape[0]
    chips = count // 2
    rows_here = count * row_dev
    rows_half = chips * row_dev
    parts = 2 if depth % (2 * LANES) == 0 else 1
    anywhere = pl.BlockSpec(memory_space=pl.ANY)
    local = pl.BlockSpec(memory_space=pltpu.VMEM)
    picked, stamp = pl.pallas_call(
        functools.partial(kernel, count),
        out_shape=(
            pltpu.VMEM((nsel, row_dev), jnp.float32),
            pltpu.VMEM((1, row_dev), jnp.float32),
        ),
        in_specs=[anywhere] * 7,
        out_specs=(local, local),
        scratch_shapes=[
            pltpu.VMEM((rows_half, depth), hidden.dtype),
            pltpu.VMEM((2 * width, depth), embedding.dtype),
            pltpu.VMEM((2, rows_here), jnp.int32),
            pltpu.VMEM((1, rows_here), jnp.int32),
            pltpu.VMEM((1, rows_here), jnp.int32),
            pltpu.VMEM((1, rows_here), jnp.int32),
            pltpu.VMEM((nsel, rows_here), jnp.int32),
            pltpu.VMEM((rows_half // LANES, 16, LANES), jnp.int32),
            pltpu.VMEM((rows_half // LANES, 2 * width, LANES), jnp.float32),
            pltpu.VMEM((rows_half // LANES, 2 * width, LANES), jnp.float32),
            pltpu.VMEM((rows_half // LANES, 8, LANES), jnp.float32),
            pltpu.VMEM((chips, 8, LANES), jnp.float32),
            pltpu.SemaphoreType.DMA((7,)),
            pltpu.SemaphoreType.DMA,
            pltpu.SemaphoreType.DMA,
            pltpu.SemaphoreType.DMA((chips * parts,)),
            pltpu.SemaphoreType.DMA((chips, parts)),
            pltpu.SemaphoreType.DMA((chips,)),
            pltpu.SemaphoreType.DMA((chips,)),
        ],
        compiler_params=pltpu.CompilerParams(collective_id=0, has_side_effects=True),
        name="decode_step",
    )(
        hidden,
        embedding,
        prev_tokens,
        last_stamp[None, :],
        sample_begin[None, :],
        seq_length[None, :],
        chosen,
    )
    picked, stamp = pl.pallas_call(
        emit,
        out_shape=(
            jax.ShapeDtypeStruct((nsel, row_dev), jnp.float32),
            jax.ShapeDtypeStruct((1, row_dev), jnp.float32),
        ),
        in_specs=[local, local],
        out_specs=(anywhere, anywhere),
        scratch_shapes=[pltpu.SemaphoreType.DMA((2,))],
        name="emit",
    )(
        pltpu.with_memory_space_constraint(picked, pltpu.VMEM),
        pltpu.with_memory_space_constraint(stamp, pltpu.VMEM),
    )
    return picked, stamp[0]


def solution(mesh):
    placed = (
        P(("groups", "vocab"), None),
        P("vocab", None),
        P(None, "groups"),
        P("groups"),
        P("groups"),
        P("groups"),
        P(None, "groups"),
    )
    return jax.shard_map(
        per_device,
        mesh=mesh,
        in_specs=placed,
        out_specs=(P(None, ("groups", "vocab")), P(("groups", "vocab"))),
        check_vma=False,
    )
```
